8 devices in a mesh: stage: 1 (over z), data: 8 (over y, x, core).
Axes of the slice: x: 2, y: 2, z: 1, core: 2. Of those that a mesh axis runs over, the one named last changes fastest.
Arguments:
- w_master: float32 [32, 2048, 1408], P('stage', 'data')
- momentum: float32 [32, 2048, 1408], P('stage', 'data')
- grad: bfloat16 [32, 2048, 1408], P('stage', 'data')
Outputs:
- output 1: bfloat16 [32, 2048, 1408], P('stage')
- output 2: float32 [32, 2048, 1408], P('stage', 'data')
All inputs are finite; a program needn't handle non-finite values.
Results may differ from the reference program's by a relative error of at most 0.00743556.
Values are sent between devices in bfloat16 or wider.
A program may use at most 1.5 GiB of HBM per device.

```python
import math
import jax
import jax.numpy as jnp
from jax import lax

DATA_DEVS = 8
MATS_DEV = 4
D = 2048
FF_E = 1408
NS_ITERS = 5

MOMENTUM = 0.95
LEARN_RATE = 0.02
WEIGHT_DECAY = 0.1
NORM_EPS = 1e-7
COEF_A = 3.4445
COEF_B = -4.7750
COEF_C = 2.0315
RMS_SCALE = 0.2 * math.sqrt(max(D, FF_E))


def setup_inputs(seed: int = 0, part: int = 0) -> dict:
    mat_count = MATS_DEV * DATA_DEVS
    key = jax.random.fold_in(jax.random.key(seed), part)
    keys = jax.random.split(key, 7)
    w_master = 0.02 * jax.random.normal(keys[0], (mat_count, D, FF_E), jnp.float32)
    left_fac = jax.random.normal(keys[1], (mat_count, D, 4), jnp.float32)
    right_fac = jax.random.normal(keys[2], (mat_count, 4, FF_E), jnp.float32)
    shared = 0.25 * jnp.einsum("mdr,mrf->mdf", left_fac, right_fac)
    row_scale = jax.random.uniform(keys[3], (mat_count, D, 1), jnp.float32, 0.5, 2.0)
    momentum = row_scale * (jax.random.normal(keys[4], (mat_count, D, FF_E), jnp.float32) + shared)
    grad_scale = jax.random.uniform(keys[5], (mat_count, D, 1), jnp.float32, 0.5, 2.0)
    grad = (grad_scale * jax.random.normal(keys[6], (mat_count, D, FF_E), jnp.float32)).astype(jnp.bfloat16)
    return {"w_master": w_master, "momentum": momentum, "grad": grad}


def newton_schulz(x_mat):
    for iteration in range(NS_ITERS):
        gram_mat = jnp.dot(x_mat, x_mat.T, preferred_element_type=jnp.float32).astype(jnp.bfloat16)
        square = jnp.dot(gram_mat, gram_mat, preferred_element_type=jnp.float32)
        poly_mat = (COEF_B * gram_mat.astype(jnp.float32) + COEF_C * square).astype(jnp.bfloat16)
        prod_mat = jnp.dot(poly_mat, x_mat, preferred_element_type=jnp.float32)
        x_mat = (COEF_A * x_mat.astype(jnp.float32) + prod_mat).astype(jnp.bfloat16)
    return x_mat


def orthogonalize(mom_one):
    frob_norm = jnp.sqrt(jnp.sum(mom_one * mom_one))
    x_mat = (mom_one.astype(jnp.bfloat16).astype(jnp.float32) / (frob_norm + NORM_EPS)).astype(jnp.bfloat16)
    if D > FF_E:
        x_mat = newton_schulz(x_mat.T).T
    else:
        x_mat = newton_schulz(x_mat)
    return x_mat.astype(jnp.float32) * RMS_SCALE


def reference(w_master, momentum, grad):
    mom_new = MOMENTUM * momentum + grad.astype(jnp.float32)

    def update_one(w_and_m):
        w_one, mom_one = w_and_m
        w_new = w_one - LEARN_RATE * (orthogonalize(mom_one) + WEIGHT_DECAY * w_one)
        return w_new.astype(jnp.bfloat16)

    params = lax.map(update_one, (w_master, mom_new))
    return params, mom_new
```

```python
import math
import jax
import jax.numpy as jnp
from jax import lax
from jax.experimental import pallas as pl
from jax.sharding import PartitionSpec as P

NS_ITERS = 5
MOMENTUM = 0.95
LEARN_RATE = 0.02
WEIGHT_DECAY = 0.1
NORM_EPS = 1e-7
COEF_A = 3.4445
COEF_B = -4.7750
COEF_C = 2.0315
COPY_ROWS = 1024
LAST_SPLIT = 6


def after(value, *deps):
    return lax.optimization_barrier((value, *deps))[0]


def ns_step(x_mat):
    wide = x_mat.shape[0] <= x_mat.shape[1]
    eq = "ip,jp->ij" if wide else "pi,pj->ij"
    gram_mat = jnp.einsum(eq, x_mat, x_mat, preferred_element_type=jnp.float32).astype(jnp.bfloat16)
    square = jnp.dot(gram_mat, gram_mat, preferred_element_type=jnp.float32)
    poly_mat = (COEF_B * gram_mat.astype(jnp.float32) + COEF_C * square).astype(jnp.bfloat16)
    poly_mat = lax.optimization_barrier(poly_mat)
    eq = "ij,jp->ip" if wide else "ij,pj->pi"
    prod_mat = jnp.einsum(eq, poly_mat, x_mat, preferred_element_type=jnp.float32)
    return (COEF_A * x_mat.astype(jnp.float32) + prod_mat).astype(jnp.bfloat16)


def momentum_body(*refs):
    mom_ref, grad_ref = refs[:2]
    new_ref, low_ref, sum_ref = refs[-3:]
    new = MOMENTUM * mom_ref[...] + grad_ref[...].astype(jnp.float32)
    new_ref[...] = new
    low_ref[...] = new.astype(jnp.bfloat16)
    sum_ref[...] = jnp.broadcast_to(jnp.sum(new * new), sum_ref.shape)


def momentum_rows(mom_rows, grad_rows, whole, first, waves, group):
    total, rows, cols = mom_rows.shape
    here = pl.BlockSpec((1, rows, cols), lambda k, d: (first + k * group + d, 0, 0))
    in_specs, operands, aliases = [here, here], [mom_rows, grad_rows], {}
    if whole is not None:
        in_specs.append(pl.BlockSpec(memory_space=pl.ANY))
        operands.append(whole)
        aliases = {2: 0}
    count = waves * group
    return pl.pallas_call(
        momentum_body,
        grid=(waves, group),
        in_specs=in_specs,
        out_specs=(
            here,
            pl.BlockSpec((1, rows, cols), lambda k, d: (d * waves + k, 0, 0)),
            pl.BlockSpec((1, 8, 128), lambda k, d: (d * waves + k, 0, 0)),
        ),
        out_shape=(
            jax.ShapeDtypeStruct((total, rows, cols), jnp.float32),
            jax.ShapeDtypeStruct((count, rows, cols), jnp.bfloat16),
            jax.ShapeDtypeStruct((count, 8, 128), jnp.float32),
        ),
        input_output_aliases=aliases,
        cost_estimate=pl.CostEstimate(flops=4 * count * rows * cols, bytes_accessed=12 * count * rows * cols, transcendentals=0),
    )(*operands)


def place_body(*refs):
    refs[-1][...] = refs[0][...]


def place(whole, piece, first, total):
    mats, rows, cols = piece.shape
    step = math.gcd(rows, COPY_ROWS)
    in_specs = [pl.BlockSpec((1, step, cols), lambda i, j: (i, j, 0))]
    operands = [piece]
    aliases = {}
    if whole is not None:
        in_specs.append(pl.BlockSpec(memory_space=pl.ANY))
        operands.append(whole)
        aliases = {1: 0}
    return pl.pallas_call(
        place_body,
        grid=(mats, rows // step),
        in_specs=in_specs,
        out_specs=pl.BlockSpec((1, step, cols), lambda i, j: (i + first, j, 0)),
        out_shape=jax.ShapeDtypeStruct((total, rows, cols), piece.dtype),
        input_output_aliases=aliases,
        cost_estimate=pl.CostEstimate(flops=2 * piece.size, bytes_accessed=4 * piece.size, transcendentals=0),
    )(*operands)


def solution(mesh):
    group = mesh.shape["data"]
    row_spec = P("stage", "data", None)
    full_spec = P("stage", None, None)

    def local_step(w_rows, mom_rows, grad_rows):
        mat_count, rows_dev, col_count = mom_rows.shape
        waves = mat_count // group
        rest = waves - 1
        rows_all = rows_dev * group
        rms_scale = 0.2 * math.sqrt(max(rows_all, col_count))

        def exchange(array):
            return lax.all_to_all(array, "data", 0, 0, tiled=True)

        mom_new, low_0, sum_0 = momentum_rows(mom_rows, grad_rows, None, 0, 1, group)
        mom_new, low_r, sum_r = momentum_rows(mom_rows, grad_rows, mom_new, group, rest, group)
        sum_0 = exchange(sum_0)
        low_0 = exchange(after(low_0, sum_0))
        sum_r = exchange(after(sum_r, low_0))
        low_r = exchange(after(low_r, sum_r)).reshape(group, rest, rows_dev, col_count)
        sum_r = sum_r.reshape(group, rest, 8, 128)

        def begin(wave):
            low, part = (low_0, sum_0[:, 0, 0]) if wave == 0 else (low_r[:, wave - 1], sum_r[:, wave - 1, 0, 0])
            whole = low.reshape(rows_all, col_count).astype(jnp.float32)
            return (whole / (jnp.sqrt(jnp.sum(part)) + NORM_EPS)).astype(jnp.bfloat16)

        def finish(x_mat, wave):
            ortho = exchange(x_mat.reshape(group, rows_dev, col_count))
            w_old = lax.slice_in_dim(w_rows, wave * group, (wave + 1) * group)
            w_new = w_old - LEARN_RATE * (ortho.astype(jnp.float32) * rms_scale + WEIGHT_DECAY * w_old)
            return lax.optimization_barrier(w_new.astype(jnp.bfloat16))

        updates = {(1, 2): 0, (2, 4): 1, (3, 4): 2}
        rows_low = [None] * waves
        pieces = []
        x_mat = None
        for wave in range(waves):
            x_mat = begin(wave) if x_mat is None else after(begin(wave), x_mat)
            for iteration in range(NS_ITERS):
                if (wave, iteration) in updates:
                    x_mat = after(x_mat, rows_low[updates[wave, iteration]])
                x_mat = ns_step(x_mat)
                x_mat = lax.optimization_barrier(x_mat)
            rows_low[wave] = finish(x_mat, wave)
            cuts = (0, LAST_SPLIT, group) if wave == waves - 1 else (0, group)
            for low, high in zip(cuts, cuts[1:]):
                part = lax.slice_in_dim(rows_low[wave], low, high)
                pieces.append((wave * group + low, lax.all_gather(part, "data", axis=1, tiled=True)))
        params = None
        for first, piece in pieces:
            params = place(params, after(piece, x_mat), first, mat_count)
        return params, mom_new

    return jax.shard_map(local_step, mesh=mesh, in_specs=(row_spec, row_spec, row_spec), out_specs=(full_spec, row_spec), check_vma=False)
```

```python
import math
import jax
import jax.numpy as jnp
from jax import lax
from jax.experimental import pallas as pl
from jax.experimental.pallas import tpu as pltpu
from jax.sharding import PartitionSpec as P

NS_ITERS = 5
MOMENTUM = 0.95
LEARN_RATE = 0.02
WEIGHT_DECAY = 0.1
NORM_EPS = 1e-7
COEF_A = 3.4445
COEF_B = -4.7750
COEF_C = 2.0315

AGENDA = (
    ("ns", 0, 0), ("ns", 0, 1), ("ns", 0, 2), ("ns", 0, 3), ("ns", 0, 4), ("out", 0),
    ("ns", 1, 0), ("ns", 1, 1), ("upd", 0), ("ns", 1, 2), ("ns", 1, 3), ("ns", 1, 4), ("out", 1),
    ("ns", 2, 0), ("dg", 0), ("pp", 0, 1, 0), ("pp", 0, 2, 1), ("ns", 2, 1), ("ns", 2, 2), ("pp", 0, 1, 1), ("pp", 0, 2, 0), ("ns", 2, 3), ("ns", 2, 4),
    ("upd", 1), ("out", 2), ("ns", 3, 0), ("ns", 3, 1), ("ns", 3, 2), ("pp", 0, 3, 0), ("pp", 0, 3, 1), ("ns", 3, 3), ("upd", 2), ("ns", 3, 4), ("out", 3),
    ("pl", 0, 0, 0), ("pl", 0, 0, 1), ("pl", 0, 1, 0), ("pl", 0, 1, 1), ("pl", 0, 2, 0), ("pl", 0, 2, 1), ("pl", 0, 3, 0), ("pl", 0, 3, 1),
    ("dg", 1), ("pp", 1, 1, 0), ("pp", 1, 2, 1), ("pl", 1, 0, 0), ("pl", 1, 0, 1), ("pl", 1, 1, 0),
    ("pp", 1, 1, 1), ("pp", 1, 2, 0), ("pl", 1, 2, 1), ("pl", 1, 1, 1), ("pl", 1, 2, 0),
    ("upd", 3), ("pl", 2, 0, 0), ("dg", 2), ("pp", 2, 1, 0), ("pp", 2, 2, 1), ("pl", 2, 0, 1), ("pl", 2, 1, 0),
    ("pp", 2, 1, 1), ("pp", 2, 2, 0), ("pl", 2, 2, 1), ("pl", 2, 1, 1), ("pl", 2, 2, 0),
    ("pp", 1, 3, 0), ("pp", 1, 3, 1), ("pl", 3, 0, 0), ("pl", 1, 3, 0), ("pl", 1, 3, 1),
    ("dg", 3), ("pp", 3, 1, 0), ("pp", 3, 2, 1), ("pl", 3, 0, 1), ("pl", 3, 1, 0),
    ("pp", 3, 1, 1), ("pp", 3, 2, 0), ("pl", 3, 2, 1), ("pl", 3, 1, 1), ("pl", 3, 2, 0),
    ("pp", 2, 3, 0), ("pp", 2, 3, 1), ("pl", 2, 3, 0), ("pl", 2, 3, 1),
    ("pp", 3, 3, 0), ("pp", 3, 3, 1), ("pl", 3, 3, 0), ("pl", 3, 3, 1),
)


def after(value, *deps):
    return lax.optimization_barrier((value, *deps))[0]


def ns_step(x_mat):
    wide = x_mat.shape[0] <= x_mat.shape[1]
    eq = "ip,jp->ij" if wide else "pi,pj->ij"
    gram_mat = jnp.einsum(eq, x_mat, x_mat, preferred_element_type=jnp.float32).astype(jnp.bfloat16)
    square = jnp.dot(gram_mat, gram_mat, preferred_element_type=jnp.float32)
    poly_mat = (COEF_B * gram_mat.astype(jnp.float32) + COEF_C * square).astype(jnp.bfloat16)
    poly_mat = lax.optimization_barrier(poly_mat)
    eq = "ij,jp->ip" if wide else "ij,pj->pi"
    prod_mat = jnp.einsum(eq, poly_mat, x_mat, preferred_element_type=jnp.float32)
    return (COEF_A * x_mat.astype(jnp.float32) + prod_mat).astype(jnp.bfloat16)


def momentum_body(me_ref, mom_ref, grad_ref, *refs):
    new_ref, low_ref, sum_ref = refs[-3:]
    new = MOMENTUM * mom_ref[...] + grad_ref[...].astype(jnp.float32)
    new_ref[...] = new
    low_ref[...] = new.astype(jnp.bfloat16)
    sum_ref[...] = jnp.broadcast_to(jnp.sum(new * new), sum_ref.shape)


def momentum_rows(me, mom_rows, grad_rows, whole, first, waves, group, by_distance):
    total, rows, cols = mom_rows.shape
    here = pl.BlockSpec((1, rows, cols), lambda k, d, me_ref: (first + k * group + d, 0, 0))
    in_specs, operands, aliases = [here, here], [mom_rows, grad_rows], {}
    if whole is not None:
        in_specs.append(pl.BlockSpec(memory_space=pl.ANY))
        operands.append(whole)
        aliases = {3: 0}
    count = waves * group
    if by_distance:
        low_map = lambda k, d, me_ref: (lax.bitwise_xor(d, me_ref[0]), 0, 0)
    else:
        low_map = lambda k, d, me_ref: (d * waves + k, 0, 0)
    return pl.pallas_call(
        momentum_body,
        grid_spec=pltpu.PrefetchScalarGridSpec(
            num_scalar_prefetch=1,
            grid=(waves, group),
            in_specs=in_specs,
            out_specs=(
                here,
                pl.BlockSpec((1, rows, cols), low_map),
                pl.BlockSpec((1, 8, 128), lambda k, d, me_ref: (d * waves + k, 0, 0)),
            ),
        ),
        out_shape=(
            jax.ShapeDtypeStruct((total, rows, cols), jnp.float32),
            jax.ShapeDtypeStruct((count, rows, cols), jnp.bfloat16),
            jax.ShapeDtypeStruct((count, 8, 128), jnp.float32),
        ),
        input_output_aliases=aliases,
        cost_estimate=pl.CostEstimate(flops=4 * count * rows * cols, bytes_accessed=12 * count * rows * cols, transcendentals=0),
    )(me, *operands)


def normalize_body(me_ref, norm_ref, *refs):
    out_ref = refs[-1]
    rows = refs[0].shape[1]
    for distance, piece in enumerate(refs[:-1]):
        start = pl.multiple_of(lax.bitwise_xor(me_ref[0], distance) * rows, rows)
        out_ref[pl.ds(start, rows)] = (piece[0].astype(jnp.float32) / norm_ref[0]).astype(jnp.bfloat16)


def normalize(me, norm, pieces):
    _, rows, cols = pieces[0].shape
    return pl.pallas_call(
        normalize_body,
        in_specs=[pl.BlockSpec(memory_space=pltpu.SMEM)] * 2 + [pl.BlockSpec(memory_space=pltpu.VMEM)] * len(pieces),
        out_specs=pl.BlockSpec(memory_space=pltpu.VMEM),
        out_shape=jax.ShapeDtypeStruct((rows * len(pieces), cols), jnp.bfloat16),
        cost_estimate=pl.CostEstimate(flops=8 * rows * cols, bytes_accessed=32 * rows * cols, transcendentals=0),
    )(me, norm, *pieces)


def place_body(me_ref, even_ref, odd_ref, *refs):
    out_ref = refs[-1]
    rows = even_ref.shape[1]
    swap = lax.rem(me_ref[0], 2)
    out_ref[0, pl.ds(pl.multiple_of(swap * rows, rows), rows)] = even_ref[0]
    out_ref[0, pl.ds(pl.multiple_of((1 - swap) * rows, rows), rows)] = odd_ref[0]


def place(whole, me, even, odd, pair, first, total, group):
    mats, rows, cols = even.shape
    piece = pl.BlockSpec((1, rows, cols), lambda i, me_ref: (i, 0, 0))
    in_specs, operands, aliases = [piece, piece], [even, odd], {}
    if whole is not None:
        in_specs.append(pl.BlockSpec(memory_space=pl.ANY))
        operands.append(whole)
        aliases = {3: 0}
    return pl.pallas_call(
        place_body,
        grid_spec=pltpu.PrefetchScalarGridSpec(
            num_scalar_prefetch=1,
            grid=(mats,),
            in_specs=in_specs,
            out_specs=pl.BlockSpec((1, 2 * rows, cols), lambda i, me_ref: (i + first, lax.bitwise_xor(me_ref[0] // 2, pair), 0)),
        ),
        out_shape=jax.ShapeDtypeStruct((total, rows * group, cols), even.dtype),
        input_output_aliases=aliases,
        cost_estimate=pl.CostEstimate(flops=4 * even.size, bytes_accessed=8 * even.size, transcendentals=0),
    )(me, *operands)


def solution(mesh):
    group = mesh.shape["data"]
    row_spec = P("stage", "data", None)
    full_spec = P("stage", None, None)

    def local_step(w_rows, mom_rows, grad_rows):
        mat_count, rows_dev, col_count = mom_rows.shape
        waves = mat_count // group
        rows_all = rows_dev * group
        rms_scale = 0.2 * math.sqrt(max(rows_all, col_count))

        def exchange(array):
            return lax.all_to_all(array, "data", 0, 0, tiled=True)

        def hop(array, bit):
            return lax.ppermute(array, "data", [(i, i ^ bit) for i in range(group)])

        my_index = lax.axis_index("data")
        me = my_index.astype(jnp.int32).reshape(1)
        mom_new, low_0, sum_0 = momentum_rows(me, mom_rows, grad_rows, None, 0, 1, group, False)
        mom_new, low_1, sum_1 = momentum_rows(me, mom_rows, grad_rows, mom_new, group, 2, group, False)
        mom_new, low_3, sum_3 = momentum_rows(me, mom_rows, grad_rows, mom_new, 3 * group, 1, group, True)
        part = jnp.concatenate([sum_0[:, 0, 0], sum_1[:, 0, 0], sum_3[:, 0, 0]])
        sq_total = part
        for bit in range(1, group):
            sq_total = sq_total + hop(part, bit)
        low_0 = exchange(low_0)
        low_1 = exchange(after(low_1, low_0)).reshape(group, 2, rows_dev, col_count)
        low_3 = lax.optimization_barrier(tuple(lax.slice_in_dim(low_3, r, r + 1) for r in range(group)))
        low_3 = [low_3[0]] + [hop(low_3[r], r) for r in range(1, group)]

        def begin(wave):
            place_of = (my_index, group + 2 * my_index, group + 2 * my_index + 1, 3 * group + my_index)[wave]
            norm = jnp.sqrt(lax.dynamic_slice_in_dim(sq_total, place_of, 1)) + NORM_EPS
            if wave == 3:
                return normalize(me, norm, after(tuple(low_3), state["x"]))
            low = low_0 if wave == 0 else low_1[:, wave - 1]
            return (low.reshape(rows_all, col_count).astype(jnp.float32) / norm).astype(jnp.bfloat16)

        half = group // 2

        def update(ortho, wave):
            halves = []
            for h in range(2):
                w_old = lax.slice_in_dim(w_rows, wave * group + h * half, wave * group + (h + 1) * half)
                part = lax.slice_in_dim(ortho, h * half, (h + 1) * half)
                w_new = w_old - LEARN_RATE * (part.astype(jnp.float32) * rms_scale + WEIGHT_DECAY * w_old)
                halves.append(w_new.astype(jnp.bfloat16))
            return lax.optimization_barrier(tuple(halves))

        got = {(w, h): {} for w in range(waves) for h in range(2)}
        final = {}
        state = {"x": None, "params": None}
        outs = {}

        def tie(*arrays):
            key = "x" if state["params"] is None else "params"
            state[key], *arrays = lax.optimization_barrier((state[key], *arrays))
            return arrays

        for kind, wave, *where in AGENDA:
            if kind == "ns":
                if where[0] == 0:
                    state["x"] = begin(wave) if state["x"] is None else after(begin(wave), state["x"])
                state["x"] = lax.optimization_barrier(ns_step(state["x"]))
            elif kind == "out":
                outs[wave] = exchange(final[wave].reshape(group, rows_dev, col_count))
            elif kind == "upd":
                (ortho,) = tie(outs.pop(wave))
                for h, own in enumerate(tie(*update(ortho, wave))):
                    mine = got[wave, h]
                    mine[0] = own
                    mine[1] = hop(own, 1)
                    mine[2] = hop(own, 2)
                    mine[4] = hop(own, 4)
            elif kind == "dg":
                got[wave, 0][2], got[wave, 1][4] = tie(got[wave, 0][2], got[wave, 1][4])
                got[wave, 0][6] = hop(got[wave, 0][2], 4)
                got[wave, 1][6] = hop(got[wave, 1][4], 2)
            elif kind == "pp":
                pair, h = where
                mine = got[wave, h]
                (mine[2 * pair],) = tie(mine[2 * pair])
                mine[2 * pair + 1] = hop(mine[2 * pair], 1)
            else:
                pair, h = where
                mine = got[wave, h]
                even = mine[2 * pair]
                if state["params"] is None:
                    even = after(even, state["x"])
                state["params"] = place(
                    state["params"], me, even, mine[2 * pair + 1], pair, wave * group + h * half, mat_count, group
                )
            if kind == "ns" and where[0] == NS_ITERS - 1:
                final[wave] = state["x"]
        params = state["params"]
        return params, mom_new

    return jax.shard_map(local_step, mesh=mesh, in_specs=(row_spec, row_spec, row_spec), out_specs=(full_spec, row_spec), check_vma=False)
```

```python
import functools
import math
import jax
import jax.numpy as jnp
from jax import lax
from jax.experimental import pallas as pl
from jax.experimental.pallas import tpu as pltpu
from jax.sharding import PartitionSpec as P

NS_ITERS = 5
SUM_ROWS = 32
MOMENTUM = 0.95
LEARN_RATE = 0.02
WEIGHT_DECAY = 0.1
NORM_EPS = 1e-7
COEF_A = 3.4445
COEF_B = -4.7750
COEF_C = 2.0315

CHUNKS = (((0, 4), (4, 4)),) * 3 + (((0, 3), (3, 3), (6, 1), (7, 1)),)
AGENDA = (
    ("ns", 0, 0), ("ns", 0, 1), ("ns", 0, 2), ("ns", 0, 3), ("ns", 0, 4), ("out", 0),
    ("ns", 1, 0), ("ns", 1, 1), ("upd", 0), ("ns", 1, 2), ("ns", 1, 3), ("ns", 1, 4), ("out", 1),
    ("ns", 2, 0), ("dg", 0, 0), ("pp", 0, 1, 0), ("pp", 0, 2, 1), ("ns", 2, 1), ("ns", 2, 2), ("pp", 0, 1, 1), ("pp", 0, 2, 0), ("ns", 2, 3), ("ns", 2, 4),
    ("upd", 1), ("out", 2), ("ns", 3, 0), ("ns", 3, 1), ("ns", 3, 2), ("pp", 0, 3, 0), ("pp", 0, 3, 1), ("ns", 3, 3), ("upd", 2), ("ns", 3, 4), ("out", 3),
    ("pl", 0, 0, 0), ("pl", 0, 0, 1), ("pl", 0, 1, 0), ("pl", 0, 1, 1), ("pl", 0, 2, 0), ("pl", 0, 2, 1), ("pl", 0, 3, 0), ("pl", 0, 3, 1),
    ("dg", 1, 0), ("pp", 1, 1, 0), ("pp", 1, 2, 1), ("pl", 1, 0, 0), ("pl", 1, 0, 1), ("pl", 1, 1, 0),
    ("pp", 1, 1, 1), ("pp", 1, 2, 0), ("pl", 1, 2, 1), ("pl", 1, 1, 1), ("pl", 1, 2, 0),
    ("upd", 3), ("pl", 2, 0, 0), ("dg", 2, 0), ("pp", 2, 1, 0), ("pp", 2, 2, 1), ("pl", 2, 0, 1), ("pl", 2, 1, 0),
    ("pp", 2, 1, 1), ("pp", 2, 2, 0), ("pl", 2, 2, 1), ("pl", 2, 1, 1), ("pl", 2, 2, 0),
    ("pp", 1, 3, 0), ("pp", 1, 3, 1), ("pl", 3, 0, 0), ("pl", 3, 0, 2), ("pl", 3, 0, 3), ("pl", 1, 3, 0), ("pl", 1, 3, 1),
    ("dg", 3, 0), ("pp", 3, 1, 0), ("pp", 3, 2, 1), ("pl", 3, 0, 1),
    ("dg", 3, 2), ("pp", 3, 1, 2), ("pp", 3, 2, 3), ("pl", 3, 1, 0), ("pl", 3, 2, 1), ("pl", 3, 1, 2), ("pl", 3, 2, 3),
    ("pp", 3, 1, 1), ("pp", 3, 2, 0), ("pp", 3, 1, 3), ("pp", 3, 2, 2), ("pl", 3, 1, 1), ("pl", 3, 2, 0), ("pl", 3, 1, 3), ("pl", 3, 2, 2),
    ("pp", 2, 3, 0), ("pp", 2, 3, 1), ("pl", 2, 3, 0), ("pl", 2, 3, 1),
    ("pp", 3, 3, 0), ("pp", 3, 3, 1), ("pl", 3, 3, 0), ("pl", 3, 3, 1),
    ("pp", 3, 3, 2), ("pp", 3, 3, 3), ("pl", 3, 3, 2), ("pl", 3, 3, 3),
)


def after(value, *deps):
    return lax.optimization_barrier((value, *deps))[0]


def ns_step(x_mat):
    wide = x_mat.shape[0] <= x_mat.shape[1]
    eq = "ip,jp->ij" if wide else "pi,pj->ij"
    gram_mat = jnp.einsum(eq, x_mat, x_mat, preferred_element_type=jnp.float32).astype(jnp.bfloat16)
    square = jnp.dot(gram_mat, gram_mat, preferred_element_type=jnp.float32)
    poly_mat = (COEF_B * gram_mat.astype(jnp.float32) + COEF_C * square).astype(jnp.bfloat16)
    poly_mat = lax.optimization_barrier(poly_mat)
    eq = "ij,jp->ip" if wide else "ij,pj->pi"
    prod_mat = jnp.einsum(eq, poly_mat, x_mat, preferred_element_type=jnp.float32)
    return (COEF_A * x_mat.astype(jnp.float32) + prod_mat).astype(jnp.bfloat16)


def momentum_body(outs, me_ref, mom_ref, grad_ref, *refs):
    refs = dict(zip(outs, refs[-len(outs):]))
    mats, rows, cols = mom_ref.shape
    step = math.gcd(rows, SUM_ROWS)
    for mat in range(mats):

        def some_rows(i, total):
            here = (mat, pl.ds(pl.multiple_of(i * step, step), step))
            new = MOMENTUM * mom_ref[here] + grad_ref[here].astype(jnp.float32)
            if "new" in refs:
                refs["new"][here] = new
            if "low" in refs:
                refs["low"][here] = new.astype(jnp.bfloat16)
                total = total + jnp.sum((new * new).reshape(step // 8, 8, cols), axis=0)
            return total

        total = lax.fori_loop(0, rows // step, some_rows, jnp.zeros((8, cols), jnp.float32))
        if "sum" in refs:
            refs["sum"][mat] = jnp.broadcast_to(jnp.sum(total), refs["sum"].shape[1:])


def momentum_rows(me, mom_rows, grad_rows, outs, whole, first, waves, group, by_distance=False):
    total, rows, cols = mom_rows.shape
    mats = 2 if waves == 1 and not by_distance else 1
    here = pl.BlockSpec((mats, rows, cols), lambda k, d, me_ref: ((first + k * group) // mats + d, 0, 0))
    in_specs, operands, aliases = [here, here], [mom_rows, grad_rows], {}
    if whole is not None:
        in_specs.append(pl.BlockSpec(memory_space=pl.ANY))
        operands.append(whole)
        aliases = {3: 0}
    count = waves * group
    if by_distance:
        low_map = lambda k, d, me_ref: (lax.bitwise_xor(d, me_ref[0]), 0, 0)
    else:
        low_map = lambda k, d, me_ref: (d * waves + k, 0, 0)
    specs = {
        "new": (here, jax.ShapeDtypeStruct((total, rows, cols), jnp.float32)),
        "low": (pl.BlockSpec((mats, rows, cols), low_map), jax.ShapeDtypeStruct((count, rows, cols), jnp.bfloat16)),
        "sum": (
            pl.BlockSpec((mats, 8, 128), lambda k, d, me_ref: (d * waves + k, 0, 0)),
            jax.ShapeDtypeStruct((count, 8, 128), jnp.float32),
        ),
    }
    return pl.pallas_call(
        functools.partial(momentum_body, outs),
        grid_spec=pltpu.PrefetchScalarGridSpec(
            num_scalar_prefetch=1,
            grid=(waves, group // mats),
            in_specs=in_specs,
            out_specs=[specs[name][0] for name in outs],
        ),
        out_shape=[specs[name][1] for name in outs],
        input_output_aliases=aliases,
        cost_estimate=pl.CostEstimate(flops=4 * count * rows * cols, bytes_accessed=12 * count * rows * cols, transcendentals=0),
    )(me, *operands)


def normalize_body(me_ref, norm_ref, *refs):
    out_ref = refs[-1]
    rows = refs[0].shape[1]
    for distance, piece in enumerate(refs[:-1]):
        start = pl.multiple_of(lax.bitwise_xor(me_ref[0], distance) * rows, rows)
        out_ref[pl.ds(start, rows)] = (piece[0].astype(jnp.float32) / norm_ref[0]).astype(jnp.bfloat16)


def normalize(me, norm, pieces):
    _, rows, cols = pieces[0].shape
    return pl.pallas_call(
        normalize_body,
        in_specs=[pl.BlockSpec(memory_space=pltpu.SMEM)] * 2 + [pl.BlockSpec(memory_space=pltpu.VMEM)] * len(pieces),
        out_specs=pl.BlockSpec(memory_space=pltpu.VMEM),
        out_shape=jax.ShapeDtypeStruct((rows * len(pieces), cols), jnp.bfloat16),
        cost_estimate=pl.CostEstimate(flops=8 * rows * cols, bytes_accessed=32 * rows * cols, transcendentals=0),
    )(me, norm, *pieces)


def place_body(me_ref, even_ref, odd_ref, *refs):
    out_ref = refs[-1]
    rows = even_ref.shape[1]
    swap = lax.rem(me_ref[0], 2)
    out_ref[0, pl.ds(pl.multiple_of(swap * rows, rows), rows)] = even_ref[0]
    out_ref[0, pl.ds(pl.multiple_of((1 - swap) * rows, rows), rows)] = odd_ref[0]


def place(whole, me, even, odd, pair, first, total, group):
    mats, rows, cols = even.shape
    piece = pl.BlockSpec((1, rows, cols), lambda i, me_ref: (i, 0, 0))
    in_specs, operands, aliases = [piece, piece], [even, odd], {}
    if whole is not None:
        in_specs.append(pl.BlockSpec(memory_space=pl.ANY))
        operands.append(whole)
        aliases = {3: 0}
    return pl.pallas_call(
        place_body,
        grid_spec=pltpu.PrefetchScalarGridSpec(
            num_scalar_prefetch=1,
            grid=(mats,),
            in_specs=in_specs,
            out_specs=pl.BlockSpec((1, 2 * rows, cols), lambda i, me_ref: (i + first, lax.bitwise_xor(me_ref[0] // 2, pair), 0)),
        ),
        out_shape=jax.ShapeDtypeStruct((total, rows * group, cols), even.dtype),
        input_output_aliases=aliases,
        cost_estimate=pl.CostEstimate(flops=4 * even.size, bytes_accessed=8 * even.size, transcendentals=0),
    )(me, *operands)


def solution(mesh):
    group = mesh.shape["data"]
    row_spec = P("stage", "data", None)
    full_spec = P("stage", None, None)

    def local_step(w_rows, mom_rows, grad_rows):
        mat_count, rows_dev, col_count = mom_rows.shape
        waves = mat_count // group
        rows_all = rows_dev * group
        rms_scale = 0.2 * math.sqrt(max(rows_all, col_count))

        def exchange(array):
            return lax.all_to_all(array, "data", 0, 0, tiled=True)

        def hop(array, bit):
            return lax.ppermute(array, "data", [(i, i ^ bit) for i in range(group)])

        my_index = lax.axis_index("data")
        me = my_index.astype(jnp.int32).reshape(1)
        low_0, sum_0 = momentum_rows(me, mom_rows, grad_rows, ("low", "sum"), None, 0, 1, group)
        mom_new, low_1, sum_1 = momentum_rows(me, mom_rows, grad_rows, ("new", "low", "sum"), None, group, 2, group)
        mom_new, low_3, sum_3 = momentum_rows(
            me, mom_rows, grad_rows, ("new", "low", "sum"), mom_new, 3 * group, 1, group, True
        )
        (mom_new,) = momentum_rows(me, mom_rows, grad_rows, ("new",), mom_new, 0, 1, group)
        part = jnp.concatenate([sum_0[:, 0, 0], sum_1[:, 0, 0], sum_3[:, 0, 0]])
        sq_total = part
        for bit in range(1, group):
            sq_total = sq_total + hop(part, bit)
        low_0 = exchange(low_0)
        low_1 = exchange(after(low_1, low_0)).reshape(group, 2, rows_dev, col_count)
        low_3 = lax.optimization_barrier(tuple(lax.slice_in_dim(low_3, r, r + 1) for r in range(group)))
        low_3 = [low_3[0]] + [hop(low_3[r], r) for r in range(1, group)]

        def begin(wave):
            place_of = (my_index, group + 2 * my_index, group + 2 * my_index + 1, 3 * group + my_index)[wave]
            norm = jnp.sqrt(lax.dynamic_slice_in_dim(sq_total, place_of, 1)) + NORM_EPS
            if wave == 3:
                return normalize(me, norm, after(tuple(low_3), state["x"]))
            low = low_0 if wave == 0 else low_1[:, wave - 1]
            return (low.reshape(rows_all, col_count).astype(jnp.float32) / norm).astype(jnp.bfloat16)

        def update(ortho, wave):
            parts = []
            for first, count in CHUNKS[wave]:
                w_old = lax.slice_in_dim(w_rows, wave * group + first, wave * group + first + count)
                part = lax.slice_in_dim(ortho, first, first + count)
                w_new = w_old - LEARN_RATE * (part.astype(jnp.float32) * rms_scale + WEIGHT_DECAY * w_old)
                parts.append(w_new.astype(jnp.bfloat16))
            return parts

        got = {(w, h): {} for w in range(waves) for h in range(len(CHUNKS[w]))}
        final = {}
        state = {"x": None, "params": None}
        outs = {}

        def tie(*arrays):
            key = "x" if state["params"] is None else "params"
            state[key], *arrays = lax.optimization_barrier((state[key], *arrays))
            return arrays

        for kind, wave, *where in AGENDA:
            if kind == "ns":
                if where[0] == 0:
                    state["x"] = begin(wave) if state["x"] is None else after(begin(wave), state["x"])
                state["x"] = lax.optimization_barrier(ns_step(state["x"]))
            elif kind == "out":
                outs[wave] = exchange(final[wave].reshape(group, rows_dev, col_count))
            elif kind == "upd":
                (ortho,) = tie(outs.pop(wave))
                for h, own in enumerate(tie(*update(ortho, wave))):
                    mine = got[wave, h]
                    mine[0] = own
                    mine[1] = hop(own, 1)
                    mine[2] = hop(own, 2)
                    mine[4] = hop(own, 4)
            elif kind == "dg":
                even, odd = got[wave, where[0]], got[wave, where[0] + 1]
                even[2], odd[4] = tie(even[2], odd[4])
                even[6] = hop(even[2], 4)
                odd[6] = hop(odd[4], 2)
            elif kind == "pp":
                pair, h = where
                mine = got[wave, h]
                (mine[2 * pair],) = tie(mine[2 * pair])
                mine[2 * pair + 1] = hop(mine[2 * pair], 1)
            else:
                pair, h = where
                mine = got[wave, h]
                even = mine[2 * pair]
                if state["params"] is None:
                    even = after(even, state["x"])
                state["params"] = place(
                    state["params"], me, even, mine[2 * pair + 1], pair, wave * group + CHUNKS[wave][h][0], mat_count, group
                )
            if kind == "ns" and where[0] == NS_ITERS - 1:
                final[wave] = state["x"]
        params = state["params"]
        return params, mom_new

    return jax.shard_map(local_step, mesh=mesh, in_specs=(row_spec, row_spec, row_spec), out_specs=(full_spec, row_spec), check_vma=False)
```

```python
import functools
import math
import jax
import jax.numpy as jnp
from jax import lax
from jax.experimental import pallas as pl
from jax.experimental.pallas import tpu as pltpu
from jax.sharding import PartitionSpec as P

NS_ITERS = 5
SUM_ROWS = 32
MOMENTUM = 0.95
LEARN_RATE = 0.02
WEIGHT_DECAY = 0.1
NORM_EPS = 1e-7
COEF_A = 3.4445
COEF_B = -4.7750
COEF_C = 2.0315

CHUNKS = (((0, 4), (4, 4)),) * 3 + (((0, 3), (3, 3), (6, 1), (7, 1)),)
AGENDA = (
    ("ns", 0, 0), ("ns", 0, 1), ("ns", 0, 2), ("ns", 0, 3), ("ns", 0, 4), ("out", 0),
    ("ns", 1, 0), ("ns", 1, 1), ("upd", 0), ("ns", 1, 2), ("ns", 1, 3), ("ns", 1, 4), ("out", 1),
    ("ns", 2, 0), ("dg", 0, 0), ("pp", 0, 1, 0), ("pp", 0, 2, 1), ("ns", 2, 1), ("ns", 2, 2), ("pp", 0, 1, 1), ("pp", 0, 2, 0), ("ns", 2, 3), ("ns", 2, 4),
    ("upd", 1), ("out", 2), ("ns", 3, 0), ("ns", 3, 1), ("ns", 3, 2), ("pp", 0, 3, 0), ("pp", 0, 3, 1), ("ns", 3, 3), ("upd", 2), ("ns", 3, 4), ("out", 3),
    ("pl", 0, 0, 0), ("pl", 0, 0, 1), ("pl", 0, 1, 0), ("pl", 0, 1, 1), ("pl", 0, 2, 0), ("pl", 0, 2, 1), ("pl", 0, 3, 0), ("pl", 0, 3, 1),
    ("dg", 1, 0), ("pp", 1, 1, 0), ("pp", 1, 2, 1), ("pl", 1, 0, 0), ("pl", 1, 0, 1), ("pl", 1, 1, 0),
    ("pp", 1, 1, 1), ("pp", 1, 2, 0), ("pl", 1, 2, 1), ("pl", 1, 1, 1), ("pl", 1, 2, 0),
    ("upd", 3), ("pl", 2, 0, 0), ("dg", 2, 0), ("pp", 2, 1, 0), ("pp", 2, 2, 1), ("pl", 2, 0, 1), ("pl", 2, 1, 0),
    ("pp", 2, 1, 1), ("pp", 2, 2, 0), ("pl", 2, 2, 1), ("pl", 2, 1, 1), ("pl", 2, 2, 0),
    ("pp", 1, 3, 0), ("pp", 1, 3, 1), ("pl", 3, 0, 0), ("pl", 3, 0, 2), ("pl", 3, 0, 3), ("pl", 1, 3, 0), ("pl", 1, 3, 1),
    ("dg", 3, 0), ("pp", 3, 1, 0), ("pp", 3, 2, 1), ("pl", 3, 0, 1),
    ("dg", 3, 2), ("pp", 3, 1, 2), ("pp", 3, 2, 3), ("pl", 3, 1, 0), ("pl", 3, 2, 1), ("pl", 3, 1, 2), ("pl", 3, 2, 3),
    ("pp", 3, 1, 1), ("pp", 3, 2, 0), ("pp", 3, 1, 3), ("pp", 3, 2, 2), ("pl", 3, 1, 1), ("pl", 3, 2, 0), ("pl", 3, 1, 3), ("pl", 3, 2, 2),
    ("pp", 2, 3, 0), ("pp", 2, 3, 1), ("pl", 2, 3, 0), ("pl", 2, 3, 1),
    ("pp", 3, 3, 0), ("pp", 3, 3, 1), ("pl", 3, 3, 0), ("pl", 3, 3, 1),
    ("pp", 3, 3, 2), ("pp", 3, 3, 3), ("pl", 3, 3, 2), ("pl", 3, 3, 3),
)


def after(value, *deps):
    return lax.optimization_barrier((value, *deps))[0]


def ns_step(x_mat):
    wide = x_mat.shape[0] <= x_mat.shape[1]
    eq = "ip,jp->ij" if wide else "pi,pj->ij"
    gram_mat = jnp.einsum(eq, x_mat, x_mat, preferred_element_type=jnp.float32).astype(jnp.bfloat16)
    square = jnp.dot(gram_mat, gram_mat, preferred_element_type=jnp.float32)
    poly_mat = (COEF_B * gram_mat.astype(jnp.float32) + COEF_C * square).astype(jnp.bfloat16)
    poly_mat = lax.optimization_barrier(poly_mat)
    eq = "ij,jp->ip" if wide else "ij,pj->pi"
    prod_mat = jnp.einsum(eq, poly_mat, x_mat, preferred_element_type=jnp.float32)
    return (COEF_A * x_mat.astype(jnp.float32) + prod_mat).astype(jnp.bfloat16)


def momentum_body(outs, me_ref, mom_ref, grad_ref, *refs):
    refs = dict(zip(outs, refs[-len(outs):]))
    mats, rows, cols = mom_ref.shape
    step = math.gcd(rows, SUM_ROWS) if mats > 1 else rows
    for mat in range(mats):

        def some_rows(i, total):
            here = (mat, pl.ds(pl.multiple_of(i * step, step), step))
            new = MOMENTUM * mom_ref[here] + grad_ref[here].astype(jnp.float32)
            if "new" in refs:
                refs["new"][here] = new
            if "low" in refs:
                refs["low"][here] = new.astype(jnp.bfloat16)
                total = total + jnp.sum((new * new).reshape(step // 8, 8, cols), axis=0)
            return total

        total = lax.fori_loop(0, rows // step, some_rows, jnp.zeros((8, cols), jnp.float32))
        if "sum" in refs:
            refs["sum"][mat] = jnp.broadcast_to(jnp.sum(total), refs["sum"].shape[1:])


def momentum_rows(me, mom_rows, grad_rows, outs, whole, first, waves, group, by_distance=False):
    total, rows, cols = mom_rows.shape
    mats = 2 if waves == 1 and not by_distance else 1
    here = pl.BlockSpec((mats, rows, cols), lambda k, d, me_ref: ((first + k * group) // mats + d, 0, 0))
    in_specs, operands, aliases = [here, here], [mom_rows, grad_rows], {}
    if whole is not None:
        in_specs.append(pl.BlockSpec(memory_space=pl.ANY))
        operands.append(whole)
        aliases = {3: 0}
    count = waves * group
    if by_distance:
        low_map = lambda k, d, me_ref: (lax.bitwise_xor(d, me_ref[0]), 0, 0)
    else:
        low_map = lambda k, d, me_ref: (d * waves + k, 0, 0)
    specs = {
        "new": (here, jax.ShapeDtypeStruct((total, rows, cols), jnp.float32)),
        "low": (pl.BlockSpec((mats, rows, cols), low_map), jax.ShapeDtypeStruct((count, rows, cols), jnp.bfloat16)),
        "sum": (
            pl.BlockSpec((mats, 8, 128), lambda k, d, me_ref: (d * waves + k, 0, 0)),
            jax.ShapeDtypeStruct((count, 8, 128), jnp.float32),
        ),
    }
    return pl.pallas_call(
        functools.partial(momentum_body, outs),
        grid_spec=pltpu.PrefetchScalarGridSpec(
            num_scalar_prefetch=1,
            grid=(waves, group // mats),
            in_specs=in_specs,
            out_specs=[specs[name][0] for name in outs],
        ),
        out_shape=[specs[name][1] for name in outs],
        input_output_aliases=aliases,
        cost_estimate=pl.CostEstimate(flops=4 * count * rows * cols, bytes_accessed=12 * count * rows * cols, transcendentals=0),
    )(me, *operands)


def normalize_body(me_ref, norm_ref, *refs):
    out_ref = refs[-1]
    rows = refs[0].shape[1]
    for distance, piece in enumerate(refs[:-1]):
        start = pl.multiple_of(lax.bitwise_xor(me_ref[0], distance) * rows, rows)
        out_ref[pl.ds(start, rows)] = (piece[0].astype(jnp.float32) / norm_ref[0]).astype(jnp.bfloat16)


def normalize(me, norm, pieces):
    _, rows, cols = pieces[0].shape
    return pl.pallas_call(
        normalize_body,
        in_specs=[pl.BlockSpec(memory_space=pltpu.SMEM)] * 2 + [pl.BlockSpec(memory_space=pltpu.VMEM)] * len(pieces),
        out_specs=pl.BlockSpec(memory_space=pltpu.VMEM),
        out_shape=jax.ShapeDtypeStruct((rows * len(pieces), cols), jnp.bfloat16),
        cost_estimate=pl.CostEstimate(flops=8 * rows * cols, bytes_accessed=32 * rows * cols, transcendentals=0),
    )(me, norm, *pieces)


def place_body(me_ref, even_ref, odd_ref, *refs):
    out_ref = refs[-1]
    rows = even_ref.shape[1]
    swap = lax.rem(me_ref[0], 2)
    out_ref[:, pl.ds(pl.multiple_of(swap * rows, rows), rows)] = even_ref[...]
    out_ref[:, pl.ds(pl.multiple_of((1 - swap) * rows, rows), rows)] = odd_ref[...]


def place(whole, me, even, odd, pair, first, total, group):
    mats, rows, cols = even.shape
    piece = pl.BlockSpec((mats, rows, cols), lambda i, me_ref: (i, 0, 0))
    in_specs, operands, aliases = [piece, piece], [even, odd], {}
    if whole is not None:
        in_specs.append(pl.BlockSpec(memory_space=pl.ANY))
        operands.append(whole)
        aliases = {3: 0}
    return pl.pallas_call(
        place_body,
        grid_spec=pltpu.PrefetchScalarGridSpec(
            num_scalar_prefetch=1,
            grid=(1,),
            in_specs=in_specs,
            out_specs=pl.BlockSpec((mats, 2 * rows, cols), lambda i, me_ref: (first // mats, lax.bitwise_xor(me_ref[0] // 2, pair), 0)),
        ),
        out_shape=jax.ShapeDtypeStruct((total, rows * group, cols), even.dtype),
        input_output_aliases=aliases,
        cost_estimate=pl.CostEstimate(flops=4 * even.size, bytes_accessed=8 * even.size, transcendentals=0),
    )(me, *operands)


def solution(mesh):
    group = mesh.shape["data"]
    row_spec = P("stage", "data", None)
    full_spec = P("stage", None, None)

    def local_step(w_rows, mom_rows, grad_rows):
        mat_count, rows_dev, col_count = mom_rows.shape
        waves = mat_count // group
        rows_all = rows_dev * group
        rms_scale = 0.2 * math.sqrt(max(rows_all, col_count))

        def exchange(array):
            return lax.all_to_all(array, "data", 0, 0, tiled=True)

        def hop(array, bit):
            return lax.ppermute(array, "data", [(i, i ^ bit) for i in range(group)])

        my_index = lax.axis_index("data")
        me = my_index.astype(jnp.int32).reshape(1)
        low_0, sum_0 = momentum_rows(me, mom_rows, grad_rows, ("low", "sum"), None, 0, 1, group)
        mom_new, low_1, sum_1 = momentum_rows(me, mom_rows, grad_rows, ("new", "low", "sum"), None, group, 2, group)
        mom_new, low_3, sum_3 = momentum_rows(
            me, mom_rows, grad_rows, ("new", "low", "sum"), mom_new, 3 * group, 1, group, True
        )
        (mom_new,) = momentum_rows(me, mom_rows, grad_rows, ("new",), mom_new, 0, 1, group)
        part = jnp.concatenate([sum_0[:, 0, 0], sum_1[:, 0, 0], sum_3[:, 0, 0]])
        sq_total = part
        for bit in range(1, group):
            sq_total = sq_total + hop(part, bit)
        low_0 = exchange(low_0)
        low_1 = exchange(after(low_1, low_0)).reshape(group, 2, rows_dev, col_count)
        low_3 = lax.optimization_barrier(tuple(lax.slice_in_dim(low_3, r, r + 1) for r in range(group)))
        low_3 = [low_3[0]] + [hop(low_3[r], r) for r in range(1, group)]

        def begin(wave):
            place_of = (my_index, group + 2 * my_index, group + 2 * my_index + 1, 3 * group + my_index)[wave]
            norm = jnp.sqrt(lax.dynamic_slice_in_dim(sq_total, place_of, 1)) + NORM_EPS
            if wave == 3:
                return normalize(me, norm, after(tuple(low_3), state["x"]))
            low = low_0 if wave == 0 else low_1[:, wave - 1]
            return (low.reshape(rows_all, col_count).astype(jnp.float32) / norm).astype(jnp.bfloat16)

        def update(ortho, wave):
            parts = []
            for first, count in CHUNKS[wave]:
                w_old = lax.slice_in_dim(w_rows, wave * group + first, wave * group + first + count)
                part = lax.slice_in_dim(ortho, first, first + count)
                w_new = w_old - LEARN_RATE * (part.astype(jnp.float32) * rms_scale + WEIGHT_DECAY * w_old)
                parts.append(w_new.astype(jnp.bfloat16))
            return parts

        got = {(w, h): {} for w in range(waves) for h in range(len(CHUNKS[w]))}
        final = {}
        state = {"x": None, "params": None}
        outs = {}

        def tie(*arrays):
            key = "x" if state["params"] is None else "params"
            state[key], *arrays = lax.optimization_barrier((state[key], *arrays))
            return arrays

        for kind, wave, *where in AGENDA:
            if kind == "ns":
                if where[0] == 0:
                    state["x"] = begin(wave) if state["x"] is None else after(begin(wave), state["x"])
                state["x"] = lax.optimization_barrier(ns_step(state["x"]))
            elif kind == "out":
                outs[wave] = exchange(final[wave].reshape(group, rows_dev, col_count))
            elif kind == "upd":
                (ortho,) = tie(outs.pop(wave))
                for h, own in enumerate(tie(*update(ortho, wave))):
                    mine = got[wave, h]
                    mine[0] = own
                    mine[1] = hop(own, 1)
                    mine[2] = hop(own, 2)
                    mine[4] = hop(own, 4)
            elif kind == "dg":
                even, odd = got[wave, where[0]], got[wave, where[0] + 1]
                even[2], odd[4] = tie(even[2], odd[4])
                even[6] = hop(even[2], 4)
                odd[6] = hop(odd[4], 2)
            elif kind == "pp":
                pair, h = where
                mine = got[wave, h]
                (mine[2 * pair],) = tie(mine[2 * pair])
                mine[2 * pair + 1] = hop(mine[2 * pair], 1)
            else:
                pair, h = where
                mine = got[wave, h]
                even = mine[2 * pair]
                if state["params"] is None:
                    even = after(even, state["x"])
                state["params"] = place(
                    state["params"], me, even, mine[2 * pair + 1], pair, wave * group + CHUNKS[wave][h][0], mat_count, group
                )
            if kind == "ns" and where[0] == NS_ITERS - 1:
                final[wave] = state["x"]
        params = state["params"]
        return params, mom_new

    return jax.shard_map(local_step, mesh=mesh, in_specs=(row_spec, row_spec, row_spec), out_specs=(full_spec, row_spec), check_vma=False)
```
